32 devices in a mesh: lat: 8 (over z, x), depth: 4 (over y, core).
Axes of the slice: x: 2, y: 2, z: 4, core: 2. Of those that a mesh axis runs over, the one named last changes fastest.
Arguments:
- surface: float32 [128, 4096], P('lat'), may hold values from -6 to 6
- velocity: float32 [2, 128, 4096], P(None, 'lat'), may hold values from -6 to 6
- block_map: int32 [128, 4096], P('lat'), may hold values from 0 to 15
- free_flags: int32 [128, 4096], P('lat'), may hold values 0 or 1
- block_rates: float32 [16], replicated, may hold values from 0.2 to 2
- previous_mesh: float32 [128, 64, 4096], P('lat', 'depth'), may hold values from -6 to 6
Outputs:
- new_surface: float32 [128, 4096], P('lat')
- mesh_field: float32 [128, 64, 4096], P('lat', 'depth')
- column_norm: float32 [128], P('lat')
The draws below stay inside these ranges and needn't reach their ends.
All inputs are finite; a program needn't handle non-finite values. No bound on the sum of `free_flags` on one device may be relied on, other than what follows from the above.
Results may differ from the reference program's by a relative error of at most 0.00002.
Values sent between devices are 32-bit elements; how exact they have to be, the bound alone decides.
No kernel may reach another device: no remote copies, remote signals or barrier semaphores. Data moves between devices by JAX's collectives and lax.ppermute only.
A program may use at most 64 MiB of HBM per device.

```python
import math
import jax
import jax.numpy as jnp
from jax import lax

NY = 4096
NB = 16
ITERS = 2
NX = 128
NZ = 64


def touch_ends(result, key, least, top_value):
    place = [jax.random.randint(jax.random.fold_in(key, axis), (), 0, length) for axis, length in enumerate(result.shape)]
    main_axis = result.shape.index(max(result.shape))
    next_to = place[:main_axis] + [(place[main_axis] + 1) % result.shape[main_axis]] + place[main_axis + 1:]
    return result.at[tuple(place)].set(least).at[tuple(next_to)].set(top_value)


def shard_levels(stream_key, extent, cuts, low, largest):
    loudness = 1.0
    for position, parts in cuts:
        heights = jax.random.uniform(jax.random.fold_in(jax.random.fold_in(stream_key, 6), position), (parts,), jnp.float32, low / len(cuts), largest / len(cuts))
        loudness = loudness * jnp.repeat(jnp.exp(heights), extent[position] // parts).reshape((-1,) + (1,) * (len(extent) - 1 - position))
    return loudness


def bell_draw(key, extent, width, most, split=(), held_as=jnp.bfloat16):
    level = shard_levels(key, extent, split, -0.22, 0.18) if split else 1.0
    result = jax.random.normal(key, extent, jnp.float32) * width * level
    return jnp.minimum(jnp.maximum(result, -most), most).astype(held_as)


def setup_inputs(seed: int = 0) -> dict:
    keys = jax.random.split(jax.random.key(seed), 7)
    return {
        "surface": bell_draw(keys[0], (NX, NY), 1.0, 6.0, ((0, 8),), jnp.float32),
        "velocity": bell_draw(keys[1], (2, NX, NY), 1.0, 6.0, ((1, 8),), jnp.float32),
        "block_map": touch_ends(jax.random.randint(keys[2], (NX, NY), 0, NB), jax.random.fold_in(keys[2], 1), 0, NB - 1).astype(jnp.int32),
        "free_flags": touch_ends((jax.random.randint(keys[3], (NX, NY), 0, 4) < 3).astype(jnp.int32), jax.random.fold_in(keys[3], 1), 0, 1),
        "block_rates": jnp.clip(jnp.exp(jax.random.uniform(keys[4], (NB,), jnp.float32, math.log(0.2), math.log(2.0))), 0.2, 2.0),
        "previous_mesh": bell_draw(keys[5], (NX, NZ, NY), 1.0, 6.0, ((0, 8), (1, 4)), jnp.float32),
    }


TIME_STEP = 0.5
RELAX_WEIGHT = 0.8

def relax_once(field, surface_shift):
    padded_rows = jnp.pad(field, ((1, 1), (0, 0), (0, 0)))
    across_rows = padded_rows[2:] + padded_rows[:-2]
    padded_cols = jnp.pad(field, ((0, 0), (0, 0), (1, 1)))
    across_cols = padded_cols[:, :, 2:] + padded_cols[:, :, :-2]
    upper = jnp.concatenate([surface_shift[:, None, :], field[:, :-1, :]], axis=1)
    lower = jnp.concatenate([field[:, 1:, :], jnp.zeros_like(field[:, :1, :])], axis=1)
    neighbours = across_rows + across_cols + upper + lower
    return (1.0 - RELAX_WEIGHT) * field + RELAX_WEIGHT * neighbours / 6.0

def reference(surface, velocity, block_map, free_flags, block_rates, previous_mesh):
    padded = jnp.pad(surface, 1)
    grad_rows = (padded[2:, 1:-1] - padded[:-2, 1:-1]) * 0.5
    grad_cols = (padded[1:-1, 2:] - padded[1:-1, :-2]) * 0.5
    laplace = padded[2:, 1:-1] + padded[:-2, 1:-1] + padded[1:-1, 2:] + padded[1:-1, :-2] - 4.0 * surface
    diffusivity = block_rates[block_map]
    tendency = -velocity[0] * grad_rows - velocity[1] * grad_cols + diffusivity * laplace
    new_surface = surface + TIME_STEP * free_flags.astype(jnp.float32) * tendency
    surface_shift = new_surface - surface
    layers = jnp.arange(NZ, dtype=jnp.int32)
    profile = (NZ - layers).astype(jnp.float32) / NZ
    field = previous_mesh + surface_shift[:, None, :] * profile[None, :, None]
    for sweep_index in range(ITERS):
        field = relax_once(field, surface_shift)
    column_norm = jnp.sqrt(lax.optimization_barrier(jnp.sum(field * field, axis=(1, 2))) / (NZ * NY))
    return (new_surface, field, column_norm)
```

```python
import jax
import jax.numpy as jnp
from jax import lax
from jax.experimental import pallas as pl
from jax.experimental.pallas import tpu as pltpu
from jax.sharding import PartitionSpec as P

ITERS = 2
TIME_STEP = 0.5
RELAX_WEIGHT = 0.8
KEEP = 1.0 - RELAX_WEIGHT
SHARE = RELAX_WEIGHT / 6.0
PAD = 128
TOP = 8
EDGE = 3
F32 = jnp.float32


def width_of(columns):
    return 1024 if columns % 1024 == 0 else columns


def profiles(scal, layers, total):
    depth = scal[0]
    base = (total - depth * layers).astype(F32)
    own = (base - lax.broadcasted_iota(jnp.int32, (layers, 1), 0).astype(F32)) / total
    pair = lax.broadcasted_iota(jnp.int32, (2, 1), 0).astype(F32)
    above = (base + 2.0 - pair) / total
    above = jnp.where(scal[1] == 1, 1.0, above)
    below = (base - layers - pair) / total
    below = jnp.where(scal[2] == 1, 0.0, below)
    return own, above, below


def clear_sides(ref, slot, columns):
    zeros = jnp.zeros((ref.shape[1], PAD), F32)
    ref[slot, :, pl.ds(0, PAD)] = zeros
    ref[slot, :, pl.ds(PAD + columns, PAD)] = zeros


def relaxed(src, slot, first, count, start, width):
    wide = src[slot, pl.ds(first, count), pl.ds(start, width + 2 * PAD)]
    span = width + 2 * PAD
    left = pltpu.roll(wide, 1, axis=1)[:, PAD : PAD + width]
    right = pltpu.roll(wide, span - 1, axis=1)[:, PAD : PAD + width]
    current = wide[:, PAD : PAD + width]
    here = pl.ds(start + PAD, width)
    upper = src[slot, pl.ds(first - 1, count), here]
    lower = src[slot, pl.ds(first + 1, count), here]
    before = src[slot - 1, pl.ds(first, count), here]
    after = src[slot + 1, pl.ds(first, count), here]
    return KEEP * current + SHARE * ((before + after) + (upper + lower) + (left + right))


def first_sweep(fields, swept, slot, scal, shift_row, layers, columns):
    width = width_of(columns)
    for start in range(0, columns, width):
        swept[slot, pl.ds(TOP - 1, layers + 2), pl.ds(PAD + start, width)] = relaxed(
            fields, slot, TOP - 1, layers + 2, start, width
        )

    @pl.when(scal[1] == 1)
    def _():
        swept[slot, pl.ds(TOP - 1, 1), pl.ds(PAD, columns)] = shift_row()

    @pl.when(scal[2] == 1)
    def _():
        swept[slot, pl.ds(TOP + layers, 1), pl.ds(PAD, columns)] = jnp.zeros((1, columns), F32)

    clear_sides(swept, slot, columns)


def second_sweep(swept, done, slot, place, layers, columns):
    width = width_of(columns)
    total = jnp.zeros((8, 128), F32)
    for start in range(0, columns, width):
        value = relaxed(swept, slot, TOP, layers, start, width)
        done[place, :, pl.ds(start, width)] = value
        square = value * value
        for i in range(0, layers, 8):
            for j in range(0, width, 128):
                total = total + square[i : i + 8, j : j + 128]
    return jnp.sum(total, axis=0, keepdims=True)


def middle_kernel(rows, layers, columns, total):
    slots = rows - 2
    width = width_of(columns)

    def kernel(scal, prev, shift, above, below, out, sums, raw, fields, swept, done, in_sem, out_sem):
        def fetch(slot):
            return pltpu.make_async_copy(prev.at[slot + 1], raw.at[slot], in_sem.at[slot])

        for slot in range(slots):
            fetch(slot).start()
        own_p, above_p, below_p = profiles(scal, layers, total)

        def build(slot, carry):
            fetch(slot).wait()
            for start in range(0, columns, width):
                here = pl.ds(start, width)
                there = pl.ds(PAD + start, width)
                row = shift[pl.ds(slot + 1, 1), here]
                fields[slot, pl.ds(TOP, layers), there] = raw[slot, :, here] + row * own_p
                fields[slot, pl.ds(TOP - 2, 2), there] = above[slot + 1, :, here] + row * above_p
                fields[slot, pl.ds(TOP + layers, 2), there] = below[slot + 1, :, here] + row * below_p
            clear_sides(fields, slot, columns)
            return carry

        lax.fori_loop(0, slots, build, 0)

        def sweep(slot, carry):
            first_sweep(
                fields, swept, slot, scal, lambda: shift[pl.ds(slot + 1, 1), :], layers, columns
            )
            return carry

        lax.fori_loop(1, slots - 1, sweep, 0)
        sums[...] = jnp.zeros(sums.shape, F32)

        def send(slot):
            return pltpu.make_async_copy(done.at[slot - 2], out.at[slot + 1], out_sem.at[slot - 2])

        def finish(slot, carry):
            sums[pl.ds(slot + 1, 1), :] = second_sweep(swept, done, slot, slot - 2, layers, columns)
            send(slot).start()
            return carry

        lax.fori_loop(2, slots - 2, finish, 0)
        for slot in range(2, slots - 2):
            send(slot).wait()

    return kernel


def edge_kernel(rows, layers, columns, total):
    width = width_of(columns)
    side = EDGE + 4

    def kernel(
        scal, sums_in, surface, shift_in, side_rates, edge_low, edge_high, far_low, far_high,
        small_low, small_high, above, below, held, out, sums, new_surface,
        shifts, fields, swept, done, out_sem,
    ):
        del held
        own_p, above_p, below_p = profiles(scal, layers, total)
        shifts[pl.ds(0, 1), :] = small_low[pl.ds(3, 1), :]
        shifts[pl.ds(1, 1), :] = (
            small_low[pl.ds(1, 1), :] + small_low[pl.ds(2, 1), :] * surface[pl.ds(0, 1), :]
        )
        shifts[pl.ds(2, 5), :] = shift_in[pl.ds(0, 5), :]
        shifts[pl.ds(2, 1), :] = (
            shift_in[pl.ds(0, 1), :] + side_rates[pl.ds(0, 1), :] * small_low[pl.ds(0, 1), :]
        )
        shifts[pl.ds(side, 5), :] = shift_in[pl.ds(rows - 5, 5), :]
        shifts[pl.ds(side + 4, 1), :] = (
            shift_in[pl.ds(rows - 1, 1), :] + side_rates[pl.ds(1, 1), :] * small_high[pl.ds(0, 1), :]
        )
        shifts[pl.ds(side + 5, 1), :] = (
            small_high[pl.ds(1, 1), :]
            + small_high[pl.ds(2, 1), :] * surface[pl.ds(rows - 1, 1), :]
        )
        shifts[pl.ds(side + 6, 1), :] = small_high[pl.ds(3, 1), :]
        new_surface[...] = surface[...] + shift_in[...]
        new_surface[pl.ds(0, 1), :] = surface[pl.ds(0, 1), :] + shifts[pl.ds(2, 1), :]
        new_surface[pl.ds(rows - 1, 1), :] = (
            surface[pl.ds(rows - 1, 1), :] + shifts[pl.ds(side + 4, 1), :]
        )

        def middle_part(slot, block, index, start):
            row = shifts[pl.ds(slot, 1), pl.ds(start, width)]
            fields[slot, pl.ds(TOP, layers), pl.ds(PAD + start, width)] = (
                block[index, :, pl.ds(start, width)] + row * own_p
            )
            return row

        def build_far(slot, block, index, corner):
            for start in range(0, columns, width):
                row = middle_part(slot, block, index, start)
                if corner is not None:
                    here = pl.ds(start, width)
                    there = pl.ds(PAD + start, width)
                    fields[slot, pl.ds(TOP - 1, 1), there] = (
                        corner[pl.ds(4, 1), here] + row * above_p[1:2]
                    )
                    fields[slot, pl.ds(TOP + layers, 1), there] = (
                        corner[pl.ds(5, 1), here] + row * below_p[0:1]
                    )
            clear_sides(fields, slot, columns)

        build_far(0, far_low, 0, None)
        build_far(1, far_low, 1, small_low)
        build_far(side + 5, far_high, 0, small_high)
        build_far(side + 6, far_high, 1, None)

        for base, block, row_base in ((2, edge_low, 0), (side, edge_high, rows - 5)):

            def build(index, carry, base=base, block=block, row_base=row_base):
                slot = base + index
                for start in range(0, columns, width):
                    here = pl.ds(start, width)
                    there = pl.ds(PAD + start, width)
                    row = middle_part(slot, block, index, start)
                    fields[slot, pl.ds(TOP - 2, 2), there] = (
                        above[row_base + index, :, here] + row * above_p
                    )
                    fields[slot, pl.ds(TOP + layers, 2), there] = (
                        below[row_base + index, :, here] + row * below_p
                    )
                clear_sides(fields, slot, columns)
                return carry

            lax.fori_loop(0, 5, build, 0)

        def sweep(index, carry):
            slot = jnp.where(index < 5, index + 1, index + 3)
            first_sweep(
                fields, swept, slot, scal, lambda: shifts[pl.ds(slot, 1), :], layers, columns
            )
            return carry

        lax.fori_loop(0, 10, sweep, 0)

        @pl.when(scal[3] == 1)
        def _():
            swept[1] = jnp.zeros(swept.shape[1:], F32)

        @pl.when(scal[4] == 1)
        def _():
            swept[side + 5] = jnp.zeros(swept.shape[1:], F32)

        sums[...] = sums_in[...]

        def row_of(index):
            return jnp.where(index < EDGE, index, index + rows - 2 * EDGE)

        def send(index):
            return pltpu.make_async_copy(done.at[index], out.at[row_of(index)], out_sem.at[index])

        def finish(index, carry):
            slot = jnp.where(index < EDGE, index + 2, index + side - 1)
            sums[pl.ds(row_of(index), 1), :] = second_sweep(
                swept, done, slot, index, layers, columns
            )
            send(index).start()
            return carry

        lax.fori_loop(0, 2 * EDGE, finish, 0)
        for index in range(2 * EDGE):
            send(index).wait()

    return kernel


def local_shift(surface, velocity, block_map, free_flags, block_rates):
    padded = jnp.pad(surface, 1)
    north = padded[:-2, 1:-1]
    south = padded[2:, 1:-1]
    west = padded[1:-1, :-2]
    east = padded[1:-1, 2:]
    labels = jnp.arange(block_rates.shape[0], dtype=jnp.int32)
    matches = block_map[None, :, :] == labels[:, None, None]
    diffusivity = jnp.sum(jnp.where(matches, block_rates[:, None, None], 0.0), axis=0)
    factor = TIME_STEP * free_flags.astype(F32)
    tendency = (
        -velocity[0] * ((south - north) * 0.5)
        - velocity[1] * ((east - west) * 0.5)
        + diffusivity * (north + south + east + west - 4.0 * surface)
    )
    low_rate = factor[:1] * (0.5 * velocity[0, :1] + diffusivity[:1])
    high_rate = factor[-1:] * (diffusivity[-1:] - 0.5 * velocity[0, -1:])
    return factor * tendency, jnp.concatenate([low_rate, high_rate], axis=0)


def per_device(surface, velocity, block_map, free_flags, block_rates, mesh_block):
    rows, layers, columns = mesh_block.shape
    lats = lax.axis_size("lat")
    depths = lax.axis_size("depth")
    total = layers * depths
    lat_up = [(i, i + 1) for i in range(lats - 1)]
    lat_down = [(j, i) for i, j in lat_up]
    depth_up = [(i, i + 1) for i in range(depths - 1)]
    depth_down = [(j, i) for i, j in depth_up]
    far_low = lax.ppermute(mesh_block[rows - 2 :], "lat", lat_up)
    far_high = lax.ppermute(mesh_block[:2], "lat", lat_down)
    above = lax.ppermute(mesh_block[:, layers - 2 :], "depth", depth_up)
    below = lax.ppermute(mesh_block[:, :2], "depth", depth_down)
    shift, side_rates = local_shift(surface, velocity, block_map, free_flags, block_rates)
    small_low = lax.ppermute(
        jnp.concatenate(
            [surface[-1:], shift[-1:], side_rates[1:], shift[-2:-1], above[-1, 1:], below[-1, :1]]
        ),
        "lat",
        lat_up,
    )
    small_high = lax.ppermute(
        jnp.concatenate(
            [surface[:1], shift[:1], side_rates[:1], shift[1:2], above[0, 1:], below[0, :1]]
        ),
        "lat",
        lat_down,
    )
    lat = lax.axis_index("lat")
    depth = lax.axis_index("depth")
    scal = jnp.stack(
        [
            depth,
            (depth == 0).astype(jnp.int32),
            (depth == depths - 1).astype(jnp.int32),
            (lat == 0).astype(jnp.int32),
            (lat == lats - 1).astype(jnp.int32),
        ]
    ).astype(jnp.int32)
    smem = pl.BlockSpec(memory_space=pltpu.SMEM)
    vmem = pl.BlockSpec(memory_space=pltpu.VMEM)
    anywhere = pl.BlockSpec(memory_space=pl.ANY)
    slots = rows - 2
    tall = layers + 2 * TOP
    wide = columns + 2 * PAD
    mesh_type = jax.ShapeDtypeStruct(mesh_block.shape, F32)
    sums_type = jax.ShapeDtypeStruct((rows, 128), F32)
    out, sums = pl.pallas_call(
        middle_kernel(rows, layers, columns, total),
        out_shape=(mesh_type, sums_type),
        in_specs=[smem, anywhere, vmem, vmem, vmem],
        out_specs=(anywhere, vmem),
        scratch_shapes=[
            pltpu.VMEM((slots, layers, columns), F32),
            pltpu.VMEM((slots, tall, wide), F32),
            pltpu.VMEM((slots, tall, wide), F32),
            pltpu.VMEM((slots - 4, layers, columns), F32),
            pltpu.SemaphoreType.DMA((slots,)),
            pltpu.SemaphoreType.DMA((slots - 4,)),
        ],
        cost_estimate=pl.CostEstimate(
            flops=20 * mesh_block.size, bytes_accessed=8 * mesh_block.size, transcendentals=0
        ),
        name="middle",
    )(scal, mesh_block, shift, above, below)
    side_slots = 2 * (EDGE + 4)
    out, sums, new_surface = pl.pallas_call(
        edge_kernel(rows, layers, columns, total),
        out_shape=(mesh_type, sums_type, jax.ShapeDtypeStruct(surface.shape, F32)),
        in_specs=[smem] + [vmem] * 12 + [anywhere],
        out_specs=(anywhere, vmem, vmem),
        scratch_shapes=[
            pltpu.VMEM((side_slots + 2, columns), F32),
            pltpu.VMEM((side_slots, tall, wide), F32),
            pltpu.VMEM((side_slots, tall, wide), F32),
            pltpu.VMEM((2 * EDGE, layers, columns), F32),
            pltpu.SemaphoreType.DMA((2 * EDGE,)),
        ],
        input_output_aliases={13: 0},
        cost_estimate=pl.CostEstimate(
            flops=10 * mesh_block.size, bytes_accessed=4 * mesh_block.size, transcendentals=0
        ),
        name="edges",
    )(
        scal, sums, surface, shift, side_rates, mesh_block[:5], mesh_block[rows - 5 :],
        far_low, far_high, small_low, small_high, above, below, out,
    )
    row_sums = jnp.sum(lax.psum(sums, "depth"), axis=1)
    return (new_surface, out, jnp.sqrt(row_sums / (total * columns)))


def solution(mesh):
    in_specs = (
        P("lat", None),
        P(None, "lat", None),
        P("lat", None),
        P("lat", None),
        P(),
        P("lat", "depth", None),
    )
    out_specs = (P("lat", None), P("lat", "depth", None), P("lat"))
    return jax.shard_map(
        per_device, mesh=mesh, in_specs=in_specs, out_specs=out_specs, check_vma=False
    )
```

```python
import jax
import jax.numpy as jnp
from jax import lax
from jax.experimental import pallas as pl
from jax.experimental.pallas import tpu as pltpu
from jax.sharding import PartitionSpec as P


TIME_STEP = 0.5
RELAX_WEIGHT = 0.8
KEEP = 1.0 - RELAX_WEIGHT
SHARE = RELAX_WEIGHT / 6.0
LANES = 128
TOP = 8
EDGE = 3
F32 = jnp.float32


def profiles(scal, layers, total):
    depth = scal[0]
    base = (total - depth * layers).astype(F32)
    own = (base - lax.broadcasted_iota(jnp.int32, (layers, 1), 0).astype(F32)) / total
    pair = lax.broadcasted_iota(jnp.int32, (2, 1), 0).astype(F32)
    above = (base + 2.0 - pair) / total
    above = jnp.where(scal[1] == 1, 1.0, above)
    below = (base - layers - pair) / total
    below = jnp.where(scal[2] == 1, 0.0, below)
    return own, above, below


def relaxed(src, slot, first, count, tiles, emit):
    lane = lax.broadcasted_iota(jnp.int32, (count, LANES), 1)
    zero = jnp.zeros((count, LANES), F32)
    rows = pl.ds(first, count)

    def read(j):
        if j == tiles:
            return zero, zero, zero
        value = src[slot, j, rows, :]
        return value, pltpu.roll(value, 1, axis=1), pltpu.roll(value, LANES - 1, axis=1)

    left_of = zero
    current, right_turned, left_turned = read(0)
    for j in range(tiles):
        following = read(j + 1)
        left = jnp.where(lane == 0, left_of, right_turned)
        right = jnp.where(lane == LANES - 1, following[2], left_turned)
        vertical = src[slot, j, pl.ds(first - 1, count), :] + src[slot, j, pl.ds(first + 1, count), :]
        lateral = src[slot - 1, j, rows, :] + src[slot + 1, j, rows, :]
        emit(j, KEEP * current + SHARE * ((lateral + vertical) + (left + right)))
        left_of = right_turned
        current, right_turned, left_turned = following


def first_sweep(fields, swept, slot, scal, shift_row, layers, tiles):
    def emit(j, value):
        swept[slot, j, pl.ds(TOP - 1, layers + 2), :] = value

    relaxed(fields, slot, TOP - 1, layers + 2, tiles, emit)

    @pl.when(scal[1] == 1)
    def _():
        for j in range(tiles):
            swept[slot, j, pl.ds(TOP - 1, 1), :] = shift_row(j)

    @pl.when(scal[2] == 1)
    def _():
        for j in range(tiles):
            swept[slot, j, pl.ds(TOP + layers, 1), :] = jnp.zeros((1, LANES), F32)


def second_sweep(swept, done, slot, place, layers, tiles):
    totals = [jnp.zeros((layers, LANES), F32) for _ in range(2)]

    def emit(j, value):
        done[place, :, pl.ds(LANES * j, LANES)] = value
        totals[j % 2] = totals[j % 2] + value * value

    relaxed(swept, slot, TOP, layers, tiles, emit)
    return jnp.sum(totals[0] + totals[1], axis=0, keepdims=True)


def lanes(j):
    return pl.ds(LANES * j, LANES)


def build(fields, slot, tiles, layers, row, main, above, below, profile):
    own_p, above_p, below_p = profile
    for j in range(tiles):
        shift = row(j)
        fields[slot, j, pl.ds(TOP, layers), :] = main(j) + shift * own_p
        if above is not None:
            values = above(j)
            count = values.shape[0]
            fields[slot, j, pl.ds(TOP - count, count), :] = values + shift * above_p[2 - count :]
            values = below(j)
            fields[slot, j, pl.ds(TOP + layers, count), :] = values + shift * below_p[:count]


def pack_kernel(rows):
    def kernel(block, low, high, sem):
        first = pltpu.make_async_copy(block.at[pl.ds(rows - 2, 2)], high, sem.at[0])
        second = pltpu.make_async_copy(block.at[pl.ds(0, 2)], low, sem.at[1])
        first.start()
        second.start()
        first.wait()
        second.wait()

    return kernel


def middle_kernel(rows, layers, columns, total):
    slots = rows - 2
    tiles = columns // LANES

    def kernel(scal, block, shift, above, below, out, sums, raw, fields, swept, done, in_sem, out_sem):
        def fetch(slot):
            return pltpu.make_async_copy(block.at[slot + 1], raw.at[slot], in_sem.at[slot])

        def send(slot):
            return pltpu.make_async_copy(done.at[slot - 2], out.at[slot + 1], out_sem.at[slot - 2])

        for slot in range(slots):
            fetch(slot).start()
        profile = profiles(scal, layers, total)
        sums[...] = jnp.zeros(sums.shape, F32)

        def step(slot, carry):
            fetch(slot).wait()
            build(
                fields, slot, tiles, layers,
                lambda j: shift[slot + 1, :, lanes(j)],
                lambda j: raw[slot, :, lanes(j)],
                lambda j: above[slot + 1, :, lanes(j)],
                lambda j: below[slot + 1, :, lanes(j)],
                profile,
            )

            @pl.when(slot >= 2)
            def _():
                first_sweep(
                    fields, swept, slot - 1, scal,
                    lambda j: shift[slot, :, lanes(j)], layers, tiles,
                )

            @pl.when(slot >= 4)
            def _():
                sums[pl.ds(slot - 1, 1), :] = second_sweep(
                    swept, done, slot - 2, slot - 4, layers, tiles
                )
                send(slot - 2).start()

            return carry

        lax.fori_loop(0, slots, step, 0)
        for slot in range(2, slots - 2):
            send(slot).wait()

    return kernel


def edge_kernel(rows, layers, columns, total):
    side = EDGE + 4
    tiles = columns // LANES

    def kernel(
        scal, sums_in, surface, shift_in, side_rates, block, far_low, far_high,
        small_low, small_high, above, below, held, out, sums, new_surface,
        raw, shifts, fields, swept, done, in_sem, out_sem,
    ):
        del held

        def fetch(index):
            row = jnp.where(index < 5, index, index + rows - 10)
            return pltpu.make_async_copy(block.at[row], raw.at[index], in_sem.at[index])

        for index in range(10):
            fetch(index).start()
        profile = profiles(scal, layers, total)
        shifts[0] = small_low[pl.ds(3, 1), :]
        shifts[1] = (
            small_low[pl.ds(1, 1), :] + small_low[pl.ds(2, 1), :] * surface[pl.ds(0, 1), :]
        )
        for i in range(1, 5):
            shifts[i + 2] = shift_in[pl.ds(i, 1), :]
        shifts[2] = (
            shift_in[pl.ds(0, 1), :] + side_rates[pl.ds(0, 1), :] * small_low[pl.ds(0, 1), :]
        )
        for i in range(4):
            shifts[side + i] = shift_in[pl.ds(rows - 5 + i, 1), :]
        shifts[side + 4] = (
            shift_in[pl.ds(rows - 1, 1), :] + side_rates[pl.ds(1, 1), :] * small_high[pl.ds(0, 1), :]
        )
        shifts[side + 5] = (
            small_high[pl.ds(1, 1), :]
            + small_high[pl.ds(2, 1), :] * surface[pl.ds(rows - 1, 1), :]
        )
        shifts[side + 6] = small_high[pl.ds(3, 1), :]
        new_surface[...] = surface[...] + shift_in[...]
        new_surface[pl.ds(0, 1), :] = surface[pl.ds(0, 1), :] + shifts[2]
        new_surface[pl.ds(rows - 1, 1), :] = (
            surface[pl.ds(rows - 1, 1), :] + shifts[side + 4]
        )

        def far(slot, halo, index, corner):
            build(
                fields, slot, tiles, layers,
                lambda j: shifts[slot, :, lanes(j)],
                lambda j: halo[index, :, lanes(j)],
                None if corner is None else lambda j: corner[pl.ds(4, 1), lanes(j)],
                None if corner is None else lambda j: corner[pl.ds(5, 1), lanes(j)],
                profile,
            )

        far(0, far_low, 0, None)
        far(1, far_low, 1, small_low)
        far(side + 5, far_high, 0, small_high)
        far(side + 6, far_high, 1, None)

        def near(index, carry):
            slot = index + 2
            row = jnp.where(index < 5, index, index + rows - 10)
            fetch(index).wait()
            build(
                fields, slot, tiles, layers,
                lambda j: shifts[slot, :, lanes(j)],
                lambda j: raw[index, :, lanes(j)],
                lambda j: above[row, :, lanes(j)],
                lambda j: below[row, :, lanes(j)],
                profile,
            )
            return carry

        lax.fori_loop(0, 10, near, 0)

        def sweep(index, carry):
            slot = jnp.where(index < 5, index + 1, index + 3)
            first_sweep(
                fields, swept, slot, scal, lambda j: shifts[slot, :, lanes(j)], layers, tiles
            )
            return carry

        lax.fori_loop(0, 10, sweep, 0)

        @pl.when(scal[3] == 1)
        def _():
            swept[1] = jnp.zeros(swept.shape[1:], F32)

        @pl.when(scal[4] == 1)
        def _():
            swept[side + 5] = jnp.zeros(swept.shape[1:], F32)

        sums[...] = sums_in[...]

        def row_of(index):
            return jnp.where(index < EDGE, index, index + rows - 2 * EDGE)

        def send(index):
            return pltpu.make_async_copy(done.at[index], out.at[row_of(index)], out_sem.at[index])

        def finish(index, carry):
            slot = jnp.where(index < EDGE, index + 2, index + side - 1)
            sums[pl.ds(row_of(index), 1), :] = second_sweep(
                swept, done, slot, index, layers, tiles
            )
            send(index).start()
            return carry

        lax.fori_loop(0, 2 * EDGE, finish, 0)
        for index in range(2 * EDGE):
            send(index).wait()

    return kernel


def local_shift(surface, velocity, block_map, free_flags, block_rates):
    padded = jnp.pad(surface, 1)
    north = padded[:-2, 1:-1]
    south = padded[2:, 1:-1]
    west = padded[1:-1, :-2]
    east = padded[1:-1, 2:]
    labels = jnp.arange(block_rates.shape[0], dtype=jnp.int32)
    matches = block_map[None, :, :] == labels[:, None, None]
    diffusivity = jnp.sum(jnp.where(matches, block_rates[:, None, None], 0.0), axis=0)
    factor = TIME_STEP * free_flags.astype(F32)
    tendency = (
        -velocity[0] * ((south - north) * 0.5)
        - velocity[1] * ((east - west) * 0.5)
        + diffusivity * (north + south + east + west - 4.0 * surface)
    )
    low_rate = factor[:1] * (0.5 * velocity[0, :1] + diffusivity[:1])
    high_rate = factor[-1:] * (diffusivity[-1:] - 0.5 * velocity[0, -1:])
    return factor * tendency, jnp.concatenate([low_rate, high_rate], axis=0)


def one_step(surface, velocity, block_map, free_flags, block_rates, mesh_block):
    rows, layers, columns = mesh_block.shape
    lats = lax.axis_size("lat")
    depths = lax.axis_size("depth")
    total = layers * depths
    lat_up = [(i, i + 1) for i in range(lats - 1)]
    lat_down = [(j, i) for i, j in lat_up]
    depth_up = [(i, i + 1) for i in range(depths - 1)]
    depth_down = [(j, i) for i, j in depth_up]
    smem = pl.BlockSpec(memory_space=pltpu.SMEM)
    vmem = pl.BlockSpec(memory_space=pltpu.VMEM)
    anywhere = pl.BlockSpec(memory_space=pltpu.HBM)
    pair_type = jax.ShapeDtypeStruct((2, layers, columns), F32)
    low_rows, high_rows = pl.pallas_call(
        pack_kernel(rows),
        out_shape=(pair_type, pair_type),
        in_specs=[anywhere],
        out_specs=(anywhere, anywhere),
        scratch_shapes=[pltpu.SemaphoreType.DMA((2,))],
        compiler_params=pltpu.CompilerParams(vmem_limit_bytes=60 << 20),
        name="pack",
    )(mesh_block)
    far_low = lax.ppermute(high_rows, "lat", lat_up)
    far_high = lax.ppermute(low_rows, "lat", lat_down)
    last_layers = mesh_block[:, layers - 2 :]
    first_layers = mesh_block[:, :2]
    above = lax.ppermute(last_layers, "depth", depth_up)
    below = lax.ppermute(first_layers, "depth", depth_down)
    shift, side_rates = local_shift(surface, velocity, block_map, free_flags, block_rates)
    small_low = lax.ppermute(
        jnp.concatenate(
            [surface[-1:], shift[-1:], side_rates[1:], shift[-2:-1], above[-1, 1:], below[-1, :1]]
        ),
        "lat",
        lat_up,
    )
    small_high = lax.ppermute(
        jnp.concatenate(
            [surface[:1], shift[:1], side_rates[:1], shift[1:2], above[0, 1:], below[0, :1]]
        ),
        "lat",
        lat_down,
    )
    lat = lax.axis_index("lat")
    depth = lax.axis_index("depth")
    scal = jnp.stack(
        [
            depth,
            (depth == 0).astype(jnp.int32),
            (depth == depths - 1).astype(jnp.int32),
            (lat == 0).astype(jnp.int32),
            (lat == lats - 1).astype(jnp.int32),
        ]
    ).astype(jnp.int32)
    slots = rows - 2
    tall = layers + 2 * TOP
    tiles = columns // LANES
    mesh_type = jax.ShapeDtypeStruct(mesh_block.shape, F32)
    sums_type = jax.ShapeDtypeStruct((rows, LANES), F32)
    out, sums = pl.pallas_call(
        middle_kernel(rows, layers, columns, total),
        out_shape=(mesh_type, sums_type),
        in_specs=[smem, anywhere, vmem, vmem, vmem],
        out_specs=(anywhere, vmem),
        scratch_shapes=[
            pltpu.VMEM((slots, layers, columns), F32),
            pltpu.VMEM((slots, tiles, tall, LANES), F32),
            pltpu.VMEM((slots, tiles, tall, LANES), F32),
            pltpu.VMEM((slots - 4, layers, columns), F32),
            pltpu.SemaphoreType.DMA((slots,)),
            pltpu.SemaphoreType.DMA((slots - 4,)),
        ],
        compiler_params=pltpu.CompilerParams(vmem_limit_bytes=32 << 20),
        cost_estimate=pl.CostEstimate(
            flops=20 * mesh_block.size, bytes_accessed=8 * mesh_block.size, transcendentals=0
        ),
        name="middle",
    )(scal, mesh_block, shift[:, None, :], above, below)
    side_slots = 2 * (EDGE + 4)
    out, sums, new_surface = pl.pallas_call(
        edge_kernel(rows, layers, columns, total),
        out_shape=(mesh_type, sums_type, jax.ShapeDtypeStruct(surface.shape, F32)),
        in_specs=[smem] + [vmem] * 4 + [anywhere] + [vmem] * 6 + [anywhere],
        out_specs=(anywhere, vmem, vmem),
        scratch_shapes=[
            pltpu.VMEM((10, layers, columns), F32),
            pltpu.VMEM((side_slots, 1, columns), F32),
            pltpu.VMEM((side_slots, tiles, tall, LANES), F32),
            pltpu.VMEM((side_slots, tiles, tall, LANES), F32),
            pltpu.VMEM((2 * EDGE, layers, columns), F32),
            pltpu.SemaphoreType.DMA((10,)),
            pltpu.SemaphoreType.DMA((2 * EDGE,)),
        ],
        input_output_aliases={12: 0},
        compiler_params=pltpu.CompilerParams(vmem_limit_bytes=32 << 20),
        cost_estimate=pl.CostEstimate(
            flops=10 * mesh_block.size, bytes_accessed=4 * mesh_block.size, transcendentals=0
        ),
        name="edges",
    )(
        scal, sums, surface, shift, side_rates, mesh_block,
        far_low, far_high, small_low, small_high, above, below, out,
    )
    row_sums = jnp.sum(lax.psum(sums, "depth"), axis=1)
    return (new_surface, out, jnp.sqrt(row_sums / (total * columns)))


def solution(mesh):
    in_specs = (
        P("lat", None),
        P(None, "lat", None),
        P("lat", None),
        P("lat", None),
        P(),
        P("lat", "depth", None),
    )
    out_specs = (P("lat", None), P("lat", "depth", None), P("lat"))
    return jax.shard_map(
        one_step, mesh=mesh, in_specs=in_specs, out_specs=out_specs, check_vma=False
    )
```
